32 devices in a mesh: dp: 8 (over y, x, core), tensor: 4 (over z).
Axes of the slice: x: 2, y: 2, z: 4, core: 2. Of those that a mesh axis runs over, the one named last changes fastest.
Arguments:
- saved_input: bfloat16 [2048, 6144], P('dp', 'tensor'), may hold values from -6 to 6
- queries: bfloat16 [2048, 1024], P('dp', 'tensor'), may hold values from -8 to 8
- keys: bfloat16 [2048, 1024], P('dp', 'tensor'), may hold values from -8 to 8
- value_weight: bfloat16 [6144, 1024], P(None, 'tensor'), may hold values from -0.109375 to 0.109375
- grad_attended: bfloat16 [2048, 1024], P('dp', 'tensor'), may hold values from -6 to 6
Outputs:
- grad_input: bfloat16 [2048, 6144], P('dp', 'tensor')
- grad_value_weight: float32 [6144, 1024], P('dp', 'tensor')
- grad_queries: bfloat16 [2048, 1024], P('dp', 'tensor')
- grad_keys: bfloat16 [2048, 1024], P('dp', 'tensor')
The draws below stay inside these ranges and needn't reach their ends.
All inputs are finite; a program needn't handle non-finite values.
Results may differ from the reference program's by a relative error of at most 0.02.
Values may be sent and summed in bfloat16 or wider, within the bound.
No kernel may reach another device: no remote copies, remote signals or barrier semaphores. Data moves between devices by JAX's collectives and lax.ppermute only.
A program may use at most 64 MiB of HBM per device.

```python
import jax
import jax.numpy as jnp
from jax import lax

D = 6144
HD = 128
HEADS_DEV = 2
SEQ = 256
HEADS = 8
GROUPS = 8
TOKENS = 2048


def paired_fields(key):
    query_seed, key_seed = jax.random.split(jax.random.fold_in(key, 7919))
    field_shape = (TOKENS, HEADS, HD)
    query_field = jax.random.truncated_normal(query_seed, -5.0, 5.0, field_shape, jnp.float32)
    key_field = jax.random.truncated_normal(key_seed, -5.0, 5.0, field_shape, jnp.float32)
    total_width = HEADS * HD
    return (query_field.reshape(TOKENS, total_width).astype(jnp.bfloat16), key_field.reshape(TOKENS, total_width).astype(jnp.bfloat16))


def draw_queries(key, part):
    return paired_fields(key)[0]


def draw_keys(key, part):
    return paired_fields(key)[1]


def strengthened(drawn, rng, source, target, parts, factor):
    owner, partner = [(jnp.arange(drawn.shape[dim]) // (drawn.shape[dim] // parts)).reshape([-1 if axis == dim else 1 for axis in range(drawn.ndim)]) for dim in (source, target)]
    chosen = jax.random.permutation(rng, parts)[partner]
    strong = (owner == chosen) | (owner == (partner + parts // 2) % parts)
    return jnp.where(strong, factor * drawn, drawn)


def block_levels(key, dims, cuts, low, largest):
    factor_of, own = 1.0, jax.random.fold_in(key, 6)
    for axis_at, blocks in cuts:
        steps = jnp.exp(jax.random.uniform(jax.random.fold_in(own, axis_at), (blocks,), jnp.float32, low / len(cuts), largest / len(cuts)))
        factor_of = factor_of * jnp.repeat(steps, dims[axis_at] // blocks).reshape([-1 if axis == axis_at else 1 for axis in range(len(dims))])
    return factor_of


def bell_draw(key, shape, width, reach, shards=(), kind=jnp.bfloat16):
    loudness = block_levels(key, shape, shards, -0.22, 0.18) if shards else 1.0
    values = jax.random.normal(key, shape, jnp.float32) * width * loudness
    return jnp.minimum(jnp.maximum(values, -reach), reach).astype(kind)


def bell_draw_with(rng, extent, width, most, shards, heavy, kind=jnp.bfloat16):
    entries = width * jax.random.normal(rng, extent, jnp.float32)
    if shards:
        entries = entries * block_levels(rng, extent, shards, -0.22, 0.18)
    return jnp.clip(strengthened(entries, jax.random.fold_in(rng, 3), *heavy), -most, most).astype(kind)


def setup_inputs(seed: int = 0) -> dict:
    key_list = jax.random.split(jax.random.key(seed), 6)
    saved_input = bell_draw_with(key_list[0], (TOKENS, D), 1.0, 6.0, ((0, 8), (1, 4)), (0, 1, 8, 2.0))
    queries = draw_queries(jax.random.fold_in(key_list[5], 71), 0)
    keys = draw_keys(jax.random.fold_in(key_list[5], 71), 0)
    value_weight = bell_draw_with(key_list[3], (D, HEADS * HD), D ** -0.5, 0.109375, ((1, 4),), (1, 0, 4, 2.0))
    grad_attended = bell_draw(key_list[4], (TOKENS, HEADS * HD), 1.0, 6.0, ((0, 8), (1, 4)))
    return dict(saved_input=saved_input, queries=queries, keys=keys, value_weight=value_weight, grad_attended=grad_attended)


def attention_backward(group_query, group_key, group_values, group_grad, causal):
    score_scale = 1.0 / jnp.sqrt(jnp.float32(HD))
    query_heads = group_query.astype(jnp.float32).reshape(SEQ, HEADS, HD)
    key_heads = group_key.astype(jnp.float32).reshape(SEQ, HEADS, HD)
    value_heads = group_values.astype(jnp.float32).reshape(SEQ, HEADS, HD)
    grad_heads = group_grad.astype(jnp.float32).reshape(SEQ, HEADS, HD)
    scores = jnp.einsum('qhd,khd->hqk', query_heads, key_heads) * score_scale
    scores = jnp.where(causal[None], scores, -jnp.inf)
    row_max = lax.optimization_barrier(jnp.max(scores, axis=-1, keepdims=True))
    weights_exp = jnp.exp(scores - row_max)
    attention = weights_exp / lax.optimization_barrier(jnp.sum(weights_exp, axis=-1, keepdims=True))
    probs_half = attention.astype(jnp.bfloat16).astype(jnp.float32)
    grad_values = jnp.einsum('hqk,qhd->khd', probs_half, grad_heads).astype(jnp.bfloat16)
    grad_probs = jnp.einsum('qhd,khd->hqk', grad_heads, value_heads)
    row_dot = lax.optimization_barrier(jnp.sum(attention * grad_probs, axis=-1, keepdims=True))
    grad_scores = (attention * (grad_probs - row_dot) * score_scale).astype(jnp.bfloat16).astype(jnp.float32)
    grad_queries = jnp.einsum('hqk,khd->qhd', grad_scores, key_heads).astype(jnp.bfloat16)
    grad_keys = jnp.einsum('hqk,qhd->khd', grad_scores, query_heads).astype(jnp.bfloat16)
    total_width = HEADS * HD
    return (grad_values.reshape(SEQ, total_width), grad_queries.reshape(SEQ, total_width), grad_keys.reshape(SEQ, total_width))

def reference(saved_input, queries, keys, value_weight, grad_attended):
    total_width = HEADS * HD
    block_width = HEADS_DEV * HD
    block_count = total_width // block_width
    weight_blocks = value_weight.astype(jnp.float32).reshape(D, block_count, block_width)
    positions = jnp.arange(SEQ)
    causal = positions[:, None] >= positions[None, :]

    def one_group(total, inputs):
        group_input, group_query, group_key, group_grad = inputs
        values = jnp.dot(group_input, value_weight, preferred_element_type=jnp.float32).astype(jnp.bfloat16)
        grad_values, grad_queries, grad_keys = attention_backward(group_query, group_key, values, group_grad, causal)
        value_blocks = grad_values.astype(jnp.float32).reshape(SEQ, block_count, block_width)
        partial_value = jnp.einsum('tnc,dnc->ntd', value_blocks, weight_blocks)
        partial_value = lax.optimization_barrier(partial_value.astype(jnp.bfloat16)).astype(jnp.float32)
        grad_input = lax.optimization_barrier(jnp.sum(partial_value, axis=0)).astype(jnp.bfloat16)
        weight_term = jnp.dot(group_input.T, grad_values, preferred_element_type=jnp.float32)
        weight_term = lax.optimization_barrier(weight_term.astype(jnp.bfloat16)).astype(jnp.float32)
        return (total + weight_term, (grad_input, grad_queries, grad_keys))
    stacked = (saved_input.reshape(GROUPS, SEQ, D), queries.reshape(GROUPS, SEQ, total_width), keys.reshape(GROUPS, SEQ, total_width), grad_attended.reshape(GROUPS, SEQ, total_width))
    total, results = lax.scan(one_group, jnp.zeros((D, total_width), jnp.float32), stacked)
    grad_input, grad_queries, grad_keys = results
    grad_value_weight = total / jnp.float32(GROUPS)
    return (grad_input.reshape(TOKENS, D), grad_value_weight, grad_queries.reshape(TOKENS, total_width), grad_keys.reshape(TOKENS, total_width))
```

```python
import jax
import jax.numpy as jnp
from jax import lax
from jax.experimental import pallas as pl
from jax.experimental.pallas import tpu as pltpu
from jax.sharding import PartitionSpec as P

HD = 128
F32 = jnp.float32
BF16 = jnp.bfloat16


def dot(a, b, ca, cb):
    return lax.dot_general(a, b, (((ca,), (cb,)), ((), ())), preferred_element_type=F32)


def head_cols(h):
    return slice(h * HD, (h + 1) * HD)


def probs_kernel(q_ref, k_ref, g_ref, att_ref, gv_ref):
    tokens, width = q_ref.shape
    scale = 1.0 / jnp.sqrt(F32(HD))
    rows = lax.broadcasted_iota(jnp.int32, (tokens, tokens), 0)
    cols = lax.broadcasted_iota(jnp.int32, (tokens, tokens), 1)
    causal = rows >= cols
    for h in range(width // HD):
        c = head_cols(h)
        scores = jnp.where(causal, dot(q_ref[:, c], k_ref[:, c], 1, 1) * scale, -jnp.inf)
        e = jnp.exp(scores - jnp.max(scores, axis=-1, keepdims=True))
        att = e / jnp.sum(e, axis=-1, keepdims=True)
        att_ref[h] = att
        gv_ref[:, c] = dot(att.astype(BF16), g_ref[:, c], 0, 0).astype(BF16)


def grads_kernel(*refs):
    att_ref, q_ref, k_ref, g_ref = refs[:4]
    parts = refs[4:-2]
    dq_ref, dk_ref = refs[-2:]
    width = q_ref.shape[1]
    scale = 1.0 / jnp.sqrt(F32(HD))
    for h in range(width // HD):
        c = head_cols(h)
        v = parts[0][:, c].astype(F32)
        for part in parts[1:]:
            v = v + part[:, c].astype(F32)
        att = att_ref[h]
        gp = dot(g_ref[:, c], v.astype(BF16), 1, 1)
        row_dot = jnp.sum(att * gp, axis=-1, keepdims=True)
        gs = (att * (gp - row_dot) * scale).astype(BF16)
        dq_ref[:, c] = dot(gs, k_ref[:, c], 1, 0).astype(BF16)
        dk_ref[:, c] = dot(gs, q_ref[:, c], 0, 0).astype(BF16)


def probs_and_grad_values(q, k, g):
    tokens, width = q.shape
    return pl.pallas_call(
        probs_kernel,
        out_shape=(
            jax.ShapeDtypeStruct((width // HD, tokens, tokens), F32),
            jax.ShapeDtypeStruct((tokens, width), BF16),
        ),
        name="probs",
    )(q, k, g)


def query_key_grads(att, q, k, g, parts):
    out = jax.ShapeDtypeStruct(q.shape, BF16)
    return pl.pallas_call(grads_kernel, out_shape=(out, out), name="qk_grads")(att, q, k, g, *parts)


def pick(bit, zero, one):
    return jnp.where(bit == 0, zero, one)


def swap(x, axis, mask):
    n = lax.axis_size(axis)
    return lax.ppermute(x, axis, [(i, i ^ mask) for i in range(n)])


def by_shared_weights(saved_input, queries, keys, value_weight, grad_attended):
    nd, nt = lax.axis_size("dp"), lax.axis_size("tensor")
    d, t = lax.axis_index("dp"), lax.axis_index("tensor")
    levels = nt.bit_length() - 1
    core = d & 1
    features, width = value_weight.shape
    mine = features // nt
    piece = mine // (2 * nd)
    bits = list(range(1, levels + 1))
    orders = (bits, bits[::-1])

    shards = []
    for half, order in enumerate(orders):
        start = half * (mine // 2) + (d & 1) * (mine // 4)
        step = mine // 4
        for bit in order:
            step //= 2
            start = start + ((d >> bit) & 1) * step
        blocks = []
        for j in range(nt):
            rows = lax.dynamic_slice(value_weight, ((t ^ j) * mine + start, 0), (piece, width))
            blocks.append(rows if j == 0 else swap(rows, "tensor", j))
        shards.append(jnp.concatenate(blocks, axis=1))

    att, grad_values = probs_and_grad_values(queries, keys, grad_attended)
    all_grads = jnp.concatenate(
        [grad_values] + [swap(grad_values, "tensor", j) for j in range(1, nt)], axis=1
    )

    for level in range(levels):
        for half, order in enumerate(orders):
            bit = order[levels - 1 - level]
            own = shards[half]
            other = swap(own, "dp", 1 << bit)
            b = (d >> bit) & 1
            shards[half] = jnp.concatenate([pick(b, own, other), pick(b, other, own)], axis=0)
    row_blocks = []
    for half in range(2):
        own = shards[half]
        other = swap(own, "dp", 1)
        row_blocks += [pick(core, own, other), pick(core, other, own)]
    weights = jnp.concatenate(row_blocks, axis=0)

    half_rows = mine // 2
    away = lax.dynamic_slice(saved_input, (0, (1 - core) * half_rows), (saved_input.shape[0], half_rows))
    home = lax.dynamic_slice(saved_input, (0, core * half_rows), (saved_input.shape[0], half_rows))
    sent = swap(dot(away, all_grads, 0, 0).astype(BF16), "dp", 1)
    summed = dot(home, all_grads, 0, 0) + sent.astype(F32)
    tiles = []
    for half, order in enumerate(orders):
        part = summed[half * (half_rows // 2) : (half + 1) * (half_rows // 2)]
        columns = {j: part[:, j * width : (j + 1) * width] for j in range(nt)}
        flip = (nt - 1) if half else 0
        chunks = {p: columns[p ^ flip] for p in range(nt)}
        for bit in order:
            b = (d >> bit) & 1
            mask = 1 << (bit - 1)
            lows = sorted(p for p in chunks if not p & mask)
            give = jnp.concatenate([pick(b, chunks[p | mask], chunks[p]) for p in lows], axis=1)
            got = swap(give.astype(BF16), "dp", 1 << bit).astype(F32)
            chunks = {
                p: pick(b, chunks[p], chunks[p | mask]) + got[:, i * width : (i + 1) * width]
                for i, p in enumerate(lows)
            }
        (tile,) = chunks.values()
        route = []
        for di in range(nd):
            for ti in range(nt):
                to = (2 * ti + (di & 1)) * nt + ((di >> 1) ^ ti ^ flip)
                route.append((di * nt + ti, to))
        tiles.append(lax.ppermute(tile.astype(BF16), ("dp", "tensor"), route))
    grad_value_weight = jnp.concatenate(tiles, axis=0).astype(F32) / F32(nd)

    partial = dot(saved_input, weights, 1, 0)
    parts = []
    for j in range(nt):
        block = partial[:, j * width : (j + 1) * width]
        parts.append(block if j == 0 else swap(block.astype(BF16), "tensor", j))
    grad_queries, grad_keys = query_key_grads(att, queries, keys, grad_attended, parts)
    grad_input = dot(all_grads, weights, 1, 1).astype(BF16)
    return grad_input, grad_value_weight, grad_queries, grad_keys


def by_collectives(saved_input, queries, keys, value_weight, grad_attended):
    width = value_weight.shape[1]
    full_input = lax.all_gather(saved_input, "tensor", axis=1, tiled=True)
    att, grad_values = probs_and_grad_values(queries, keys, grad_attended)
    weight_part = dot(full_input, grad_values, 0, 0).astype(BF16)
    summed = lax.psum_scatter(weight_part, "dp", scatter_dimension=0, tiled=True).astype(F32)
    input_part = dot(grad_values, value_weight, 1, 1).astype(BF16)
    grad_input = lax.psum_scatter(input_part, "tensor", scatter_dimension=1, tiled=True)
    values = dot(full_input, value_weight, 1, 0)
    grad_queries, grad_keys = query_key_grads(att, queries, keys, grad_attended, [values])
    return grad_input, summed / F32(lax.axis_size("dp")), grad_queries, grad_keys


def solution(mesh):
    nd, nt = mesh.shape["dp"], mesh.shape["tensor"]

    def on_device(saved_input, *rest):
        paired = nd == 2 * nt and nt > 1 and nt & (nt - 1) == 0
        if paired and saved_input.shape[1] % (32 * nd) == 0:
            return by_shared_weights(saved_input, *rest)
        return by_collectives(saved_input, *rest)

    split = P("dp", "tensor")
    return jax.shard_map(
        on_device,
        mesh=mesh,
        in_specs=(split, split, split, P(None, "tensor"), split),
        out_specs=(split, split, split, split),
        check_vma=False,
    )
```

```python
import jax
import jax.numpy as jnp
from jax import lax
from jax.experimental import pallas as pl
from jax.sharding import PartitionSpec as P


HD = 128
F32 = jnp.float32
BF16 = jnp.bfloat16


def dot(a, b, ca, cb):
    return lax.dot_general(a, b, (((ca,), (cb,)), ((), ())), preferred_element_type=F32)


def head_cols(h):
    return slice(h * HD, (h + 1) * HD)


def probs_kernel(q_ref, k_ref, g_ref, att_ref, gv_ref):
    tokens, width = q_ref.shape
    scale = 1.0 / jnp.sqrt(F32(HD))
    rows = lax.broadcasted_iota(jnp.int32, (tokens, tokens), 0)
    cols = lax.broadcasted_iota(jnp.int32, (tokens, tokens), 1)
    causal = rows >= cols
    for h in range(width // HD):
        c = head_cols(h)
        scores = jnp.where(causal, dot(q_ref[:, c], k_ref[:, c], 1, 1) * scale, -jnp.inf)
        e = jnp.exp(scores - jnp.max(scores, axis=-1, keepdims=True))
        att = e / jnp.sum(e, axis=-1, keepdims=True)
        att_ref[h] = att
        gv_ref[:, c] = dot(att.astype(BF16), g_ref[:, c], 0, 0).astype(BF16)


def grads_kernel(*refs):
    att_ref, q_ref, k_ref, g_ref = refs[:4]
    parts = refs[4:-2]
    dq_ref, dk_ref = refs[-2:]
    width = q_ref.shape[1]
    scale = 1.0 / jnp.sqrt(F32(HD))
    for h in range(width // HD):
        c = head_cols(h)
        v = parts[0][:, c].astype(F32)
        for part in parts[1:]:
            v = v + part[:, c].astype(F32)
        att = att_ref[h]
        gp = dot(g_ref[:, c], v.astype(BF16), 1, 1)
        row_dot = jnp.sum(att * gp, axis=-1, keepdims=True)
        gs = (att * (gp - row_dot) * scale).astype(BF16)
        dq_ref[:, c] = dot(gs, k_ref[:, c], 1, 0).astype(BF16)
        dk_ref[:, c] = dot(gs, q_ref[:, c], 0, 0).astype(BF16)


def probs_and_grad_values(q, k, g):
    tokens, width = q.shape
    return pl.pallas_call(
        probs_kernel,
        out_shape=(
            jax.ShapeDtypeStruct((width // HD, tokens, tokens), F32),
            jax.ShapeDtypeStruct((tokens, width), BF16),
        ),
        name="probs",
    )(q, k, g)


def query_key_grads(att, q, k, g, parts):
    out = jax.ShapeDtypeStruct(q.shape, BF16)
    return pl.pallas_call(grads_kernel, out_shape=(out, out), name="qk_grads")(att, q, k, g, *parts)


def pick(bit, zero, one):
    return jnp.where(bit == 0, zero, one)


def swap(x, axis, mask):
    n = lax.axis_size(axis)
    return lax.ppermute(x, axis, [(i, i ^ mask) for i in range(n)])


def by_shared_weights(saved_input, queries, keys, value_weight, grad_attended):
    nd, nt = lax.axis_size("dp"), lax.axis_size("tensor")
    d, t = lax.axis_index("dp"), lax.axis_index("tensor")
    levels = nt.bit_length() - 1
    core = d & 1
    features, width = value_weight.shape
    mine = features // nt
    half_rows, quarter, piece = mine // 2, mine // 4, mine // (2 * nd)
    bits = list(range(1, levels + 1))
    orders = (bits, bits[::-1])

    starts = []
    for half, order in enumerate(orders):
        start = half * half_rows + core * quarter
        step = quarter
        for bit in order:
            step //= 2
            start = start + ((d >> bit) & 1) * step
        starts.append(start)
    blocks = []
    for j in range(nt):
        rows = jnp.concatenate(
            [
                lax.dynamic_slice(value_weight, ((t ^ j) * mine + start, 0), (piece, width))
                for start in starts
            ],
            axis=0,
        )
        blocks.append(rows if j == 0 else swap(rows, "tensor", j))
    both = jnp.concatenate(blocks, axis=1)
    shards = [both[:piece], both[piece:]]

    def input_cols(start, size):
        return lax.dynamic_slice(saved_input, (0, start), (saved_input.shape[0], size))

    pair_input = swap(input_cols((1 - core) * half_rows, half_rows), "dp", 1)
    att, grad_values = probs_and_grad_values(queries, keys, grad_attended)
    others = [swap(grad_values, "tensor", j) for j in range(1, nt)]
    all_grads = jnp.concatenate([grad_values] + others, axis=1)

    for level in range(levels):
        for half, order in enumerate(orders):
            bit = order[levels - 1 - level]
            own = shards[half]
            other = swap(own, "dp", 1 << bit)
            b = (d >> bit) & 1
            shards[half] = jnp.concatenate([pick(b, own, other), pick(b, other, own)], axis=0)
    received = [swap(own, "dp", 1) for own in shards]

    pair_grads = swap(all_grads, "dp", 1)
    home = input_cols(core * half_rows, half_rows)
    summed = dot(home, all_grads, 0, 0)
    summed = summed + dot(pair_input, pair_grads, 0, 0)
    tiles = []
    for half, order in enumerate(orders):
        part = summed[half * quarter : (half + 1) * quarter]
        columns = {j: part[:, j * width : (j + 1) * width] for j in range(nt)}
        flip = (nt - 1) if half else 0
        chunks = {p: columns[p ^ flip] for p in range(nt)}
        for bit in order:
            b = (d >> bit) & 1
            mask = 1 << (bit - 1)
            lows = sorted(p for p in chunks if not p & mask)
            give = jnp.concatenate([pick(b, chunks[p | mask], chunks[p]) for p in lows], axis=1)
            got = swap(give.astype(BF16), "dp", 1 << bit).astype(F32)
            chunks = {
                p: pick(b, chunks[p], chunks[p | mask]) + got[:, i * width : (i + 1) * width]
                for i, p in enumerate(lows)
            }
        (tile,) = chunks.values()
        route = []
        for di in range(nd):
            for ti in range(nt):
                to = (2 * ti + (di & 1)) * nt + ((di >> 1) ^ ti ^ flip)
                route.append((di * nt + ti, to))
        tiles.append(lax.ppermute(tile.astype(BF16), ("dp", "tensor"), route))
    grad_value_weight = jnp.concatenate(tiles, axis=0).astype(F32) / F32(nd)

    own_starts = [half * half_rows + core * quarter for half in range(2)]
    pair_starts = [half * half_rows + (1 - core) * quarter for half in range(2)]
    partial = sum(dot(input_cols(s, quarter), w, 1, 0) for s, w in zip(own_starts, shards))
    partial += sum(dot(input_cols(s, quarter), w, 1, 0) for s, w in zip(pair_starts, received))
    parts = []
    for j in range(nt):
        block = partial[:, j * width : (j + 1) * width]
        parts.append(block if j == 0 else swap(block.astype(BF16), "tensor", j))
    grad_queries, grad_keys = query_key_grads(att, queries, keys, grad_attended, parts)

    pieces = []
    for own_w, pair_w in zip(shards, received):
        own = dot(all_grads, own_w, 1, 1).astype(BF16)
        pair = dot(all_grads, pair_w, 1, 1).astype(BF16)
        pieces += [pick(core, own, pair), pick(core, pair, own)]
    grad_input = jnp.concatenate(pieces, axis=1)
    return grad_input, grad_value_weight, grad_queries, grad_keys


def by_collectives(saved_input, queries, keys, value_weight, grad_attended):
    full_input = lax.all_gather(saved_input, "tensor", axis=1, tiled=True)
    att, grad_values = probs_and_grad_values(queries, keys, grad_attended)
    weight_part = dot(full_input, grad_values, 0, 0).astype(BF16)
    summed = lax.psum_scatter(weight_part, "dp", scatter_dimension=0, tiled=True).astype(F32)
    input_part = dot(grad_values, value_weight, 1, 1).astype(BF16)
    grad_input = lax.psum_scatter(input_part, "tensor", scatter_dimension=1, tiled=True)
    values = dot(full_input, value_weight, 1, 0)
    grad_queries, grad_keys = query_key_grads(att, queries, keys, grad_attended, [values])
    return grad_input, summed / F32(lax.axis_size("dp")), grad_queries, grad_keys


def solution(mesh):
    nd, nt = mesh.shape["dp"], mesh.shape["tensor"]

    def on_device(saved_input, *rest):
        paired = nd == 2 * nt and nt > 1 and nt & (nt - 1) == 0
        if paired and saved_input.shape[1] % (32 * nd) == 0:
            return by_shared_weights(saved_input, *rest)
        return by_collectives(saved_input, *rest)

    split = P("dp", "tensor")
    return jax.shard_map(
        on_device,
        mesh=mesh,
        in_specs=(split, split, split, P(None, "tensor"), split),
        out_specs=(split, split, split, split),
        check_vma=False,
    )
```

```python
import jax
import jax.numpy as jnp
from jax import lax
from jax.experimental import pallas as pl
from jax.sharding import PartitionSpec as P


HD = 128
F32 = jnp.float32
BF16 = jnp.bfloat16


def dot(a, b, ca, cb):
    return lax.dot_general(a, b, (((ca,), (cb,)), ((), ())), preferred_element_type=F32)


def head_cols(h):
    return slice(h * HD, (h + 1) * HD)


def probs_kernel(q_ref, k_ref, g_ref, att_ref, gv_ref):
    tokens, width = q_ref.shape
    scale = 1.0 / jnp.sqrt(F32(HD))
    rows = lax.broadcasted_iota(jnp.int32, (tokens, tokens), 0)
    cols = lax.broadcasted_iota(jnp.int32, (tokens, tokens), 1)
    causal = rows >= cols
    for h in range(width // HD):
        c = head_cols(h)
        scores = jnp.where(causal, dot(q_ref[:, c], k_ref[:, c], 1, 1) * scale, -jnp.inf)
        e = jnp.exp(scores - jnp.max(scores, axis=-1, keepdims=True))
        att = e / jnp.sum(e, axis=-1, keepdims=True)
        att_ref[h] = att
        gv_ref[:, c] = dot(att.astype(BF16), g_ref[:, c], 0, 0).astype(BF16)


def grads_kernel(*refs):
    att_ref, q_ref, k_ref, g_ref = refs[:4]
    parts = refs[4:-2]
    dq_ref, dk_ref = refs[-2:]
    width = q_ref.shape[1]
    scale = 1.0 / jnp.sqrt(F32(HD))
    for h in range(width // HD):
        c = head_cols(h)
        v = parts[0][:, c].astype(F32)
        for part in parts[1:]:
            v = v + part[:, c].astype(F32)
        att = att_ref[h]
        gp = dot(g_ref[:, c], v.astype(BF16), 1, 1)
        row_dot = jnp.sum(att * gp, axis=-1, keepdims=True)
        gs = (att * (gp - row_dot) * scale).astype(BF16)
        dq_ref[:, c] = dot(gs, k_ref[:, c], 1, 0).astype(BF16)
        dk_ref[:, c] = dot(gs, q_ref[:, c], 0, 0).astype(BF16)


def probs_and_grad_values(q, k, g):
    tokens, width = q.shape
    return pl.pallas_call(
        probs_kernel,
        out_shape=(
            jax.ShapeDtypeStruct((width // HD, tokens, tokens), F32),
            jax.ShapeDtypeStruct((tokens, width), BF16),
        ),
        name="probs",
    )(q, k, g)


def query_key_grads(att, q, k, g, parts):
    out = jax.ShapeDtypeStruct(q.shape, BF16)
    return pl.pallas_call(grads_kernel, out_shape=(out, out), name="qk_grads")(att, q, k, g, *parts)


def pick(bit, zero, one):
    return jnp.where(bit == 0, zero, one)


def swap(x, axis, mask):
    n = lax.axis_size(axis)
    return lax.ppermute(x, axis, [(i, i ^ mask) for i in range(n)])


def by_shared_weights(saved_input, queries, keys, value_weight, grad_attended):
    nd, nt = lax.axis_size("dp"), lax.axis_size("tensor")
    d, t = lax.axis_index("dp"), lax.axis_index("tensor")
    levels = nt.bit_length() - 1
    core = d & 1
    features, width = value_weight.shape
    mine = features // nt
    half_rows, quarter, piece = mine // 2, mine // 4, mine // (2 * nd)
    bits = list(range(1, levels + 1))
    orders = (bits, bits[::-1])

    starts = []
    for half, order in enumerate(orders):
        start = half * half_rows + core * quarter
        step = quarter
        for bit in order:
            step //= 2
            start = start + ((d >> bit) & 1) * step
        starts.append(start)
    blocks = []
    for j in range(nt):
        rows = jnp.concatenate(
            [
                lax.dynamic_slice(value_weight, ((t ^ j) * mine + start, 0), (piece, width))
                for start in starts
            ],
            axis=0,
        )
        blocks.append(rows if j == 0 else swap(rows, "tensor", j))
    both = jnp.concatenate(blocks, axis=1)
    shards = [both[:piece], both[piece:]]

    def input_cols(start, size):
        return lax.dynamic_slice(saved_input, (0, start), (saved_input.shape[0], size))

    pair_input = swap(input_cols((1 - core) * half_rows, half_rows), "dp", 1)
    att, grad_values = probs_and_grad_values(queries, keys, grad_attended)
    others = [swap(grad_values, "tensor", j) for j in range(1, nt)]
    all_grads = jnp.concatenate([grad_values] + others, axis=1)

    for level in range(levels):
        for half, order in enumerate(orders):
            bit = order[levels - 1 - level]
            own = shards[half]
            other = swap(own, "dp", 1 << bit)
            b = (d >> bit) & 1
            shards[half] = jnp.concatenate([pick(b, own, other), pick(b, other, own)], axis=0)
    received = [swap(own, "dp", 1) for own in shards]

    pair_grads = swap(all_grads, "dp", 1)
    home = input_cols(core * half_rows, half_rows)
    summed = dot(home, all_grads, 0, 0)
    summed = (summed + dot(pair_input, pair_grads, 0, 0)).astype(BF16)
    tiles = []
    for half, order in enumerate(orders):
        part = summed[half * quarter : (half + 1) * quarter]
        columns = {j: part[:, j * width : (j + 1) * width] for j in range(nt)}
        flip = (nt - 1) if half else 0
        chunks = {p: columns[p ^ flip] for p in range(nt)}
        for bit in order:
            b = (d >> bit) & 1
            mask = 1 << (bit - 1)
            lows = sorted(p for p in chunks if not p & mask)
            give = jnp.concatenate([pick(b, chunks[p | mask], chunks[p]) for p in lows], axis=1)
            got = swap(give.astype(BF16), "dp", 1 << bit)
            chunks = {
                p: pick(b, chunks[p], chunks[p | mask]).astype(F32)
                + got[:, i * width : (i + 1) * width].astype(F32)
                for i, p in enumerate(lows)
            }
        (tile,) = chunks.values()
        route = []
        for di in range(nd):
            for ti in range(nt):
                to = (2 * ti + (di & 1)) * nt + ((di >> 1) ^ ti ^ flip)
                route.append((di * nt + ti, to))
        tiles.append(lax.ppermute(tile.astype(BF16), ("dp", "tensor"), route))
    grad_value_weight = jnp.concatenate(tiles, axis=0).astype(F32) / F32(nd)

    own_starts = [half * half_rows + core * quarter for half in range(2)]
    pair_starts = [half * half_rows + (1 - core) * quarter for half in range(2)]
    partial = sum(dot(input_cols(s, quarter), w, 1, 0) for s, w in zip(own_starts, shards))
    partial += sum(dot(input_cols(s, quarter), w, 1, 0) for s, w in zip(pair_starts, received))
    parts = []
    for j in range(nt):
        block = partial[:, j * width : (j + 1) * width]
        parts.append(block if j == 0 else swap(block.astype(BF16), "tensor", j))
    grad_queries, grad_keys = query_key_grads(att, queries, keys, grad_attended, parts)

    pieces = []
    for own_w, pair_w in zip(shards, received):
        own = dot(all_grads, own_w, 1, 1).astype(BF16)
        pair = dot(all_grads, pair_w, 1, 1).astype(BF16)
        pieces += [pick(core, own, pair), pick(core, pair, own)]
    grad_input = jnp.concatenate(pieces, axis=1)
    return grad_input, grad_value_weight, grad_queries, grad_keys


def by_collectives(saved_input, queries, keys, value_weight, grad_attended):
    full_input = lax.all_gather(saved_input, "tensor", axis=1, tiled=True)
    att, grad_values = probs_and_grad_values(queries, keys, grad_attended)
    weight_part = dot(full_input, grad_values, 0, 0).astype(BF16)
    summed = lax.psum_scatter(weight_part, "dp", scatter_dimension=0, tiled=True).astype(F32)
    input_part = dot(grad_values, value_weight, 1, 1).astype(BF16)
    grad_input = lax.psum_scatter(input_part, "tensor", scatter_dimension=1, tiled=True)
    values = dot(full_input, value_weight, 1, 0)
    grad_queries, grad_keys = query_key_grads(att, queries, keys, grad_attended, [values])
    return grad_input, summed / F32(lax.axis_size("dp")), grad_queries, grad_keys


def solution(mesh):
    nd, nt = mesh.shape["dp"], mesh.shape["tensor"]

    def on_device(saved_input, *rest):
        paired = nd == 2 * nt and nt > 1 and nt & (nt - 1) == 0
        if paired and saved_input.shape[1] % (32 * nd) == 0:
            return by_shared_weights(saved_input, *rest)
        return by_collectives(saved_input, *rest)

    split = P("dp", "tensor")
    return jax.shard_map(
        on_device,
        mesh=mesh,
        in_specs=(split, split, split, P(None, "tensor"), split),
        out_specs=(split, split, split, split),
        check_vma=False,
    )
```

```python
import jax
import jax.numpy as jnp
from jax import lax
from jax.experimental import pallas as pl
from jax.sharding import PartitionSpec as P


HD = 128
F32 = jnp.float32
BF16 = jnp.bfloat16


def dot(a, b, ca, cb):
    return lax.dot_general(a, b, (((ca,), (cb,)), ((), ())), preferred_element_type=F32)


def head_cols(h):
    return slice(h * HD, (h + 1) * HD)


def probs_kernel(q_ref, k_ref, g_ref, att_ref, gv_ref):
    tokens, width = q_ref.shape
    scale = 1.0 / jnp.sqrt(F32(HD))
    rows = lax.broadcasted_iota(jnp.int32, (tokens, tokens), 0)
    cols = lax.broadcasted_iota(jnp.int32, (tokens, tokens), 1)
    causal = rows >= cols
    for h in range(width // HD):
        c = head_cols(h)
        scores = jnp.where(causal, dot(q_ref[:, c], k_ref[:, c], 1, 1) * scale, -jnp.inf)
        e = jnp.exp(scores - jnp.max(scores, axis=-1, keepdims=True))
        att = e / jnp.sum(e, axis=-1, keepdims=True)
        att_ref[h] = att
        gv_ref[:, c] = dot(att.astype(BF16), g_ref[:, c], 0, 0).astype(BF16)


def grads_kernel(*refs):
    att_ref, q_ref, k_ref, g_ref = refs[:4]
    parts = refs[4:-2]
    dq_ref, dk_ref = refs[-2:]
    width = q_ref.shape[1]
    scale = 1.0 / jnp.sqrt(F32(HD))
    for h in range(width // HD):
        c = head_cols(h)
        v = parts[0][:, c].astype(F32)
        for part in parts[1:]:
            v = v + part[:, c].astype(F32)
        att = att_ref[h]
        gp = dot(g_ref[:, c], v.astype(BF16), 1, 1)
        row_dot = jnp.sum(att * gp, axis=-1, keepdims=True)
        gs = (att * (gp - row_dot) * scale).astype(BF16)
        dq_ref[:, c] = dot(gs, k_ref[:, c], 1, 0).astype(BF16)
        dk_ref[:, c] = dot(gs, q_ref[:, c], 0, 0).astype(BF16)


def probs_and_grad_values(q, k, g):
    tokens, width = q.shape
    return pl.pallas_call(
        probs_kernel,
        out_shape=(
            jax.ShapeDtypeStruct((width // HD, tokens, tokens), F32),
            jax.ShapeDtypeStruct((tokens, width), BF16),
        ),
        name="probs",
    )(q, k, g)


def query_key_grads(att, q, k, g, parts):
    out = jax.ShapeDtypeStruct(q.shape, BF16)
    return pl.pallas_call(grads_kernel, out_shape=(out, out), name="qk_grads")(att, q, k, g, *parts)


def pick(bit, zero, one):
    return jnp.where(bit == 0, zero, one)


def swap(x, axis, mask):
    n = lax.axis_size(axis)
    return lax.ppermute(x, axis, [(i, i ^ mask) for i in range(n)])


def by_shared_weights(saved_input, queries, keys, value_weight, grad_attended):
    nd, nt = lax.axis_size("dp"), lax.axis_size("tensor")
    d, t = lax.axis_index("dp"), lax.axis_index("tensor")
    levels = nt.bit_length() - 1
    core = d & 1
    features, width = value_weight.shape
    mine = features // nt
    half_rows, quarter, piece = mine // 2, mine // 4, mine // (2 * nd)
    bits = list(range(1, levels + 1))
    orders = (bits, bits[::-1])

    starts = []
    for half, order in enumerate(orders):
        start = half * half_rows + core * quarter
        step = quarter
        for bit in order:
            step //= 2
            start = start + ((d >> bit) & 1) * step
        starts.append(start)
    blocks = []
    for j in range(nt):
        rows = jnp.concatenate(
            [
                lax.dynamic_slice(value_weight, ((t ^ j) * mine + start, 0), (piece, width))
                for start in starts
            ],
            axis=0,
        )
        blocks.append(rows if j == 0 else swap(rows, "tensor", j))
    both = jnp.concatenate(blocks, axis=1)
    shards = [both[:piece], both[piece:]]

    def input_cols(start, size):
        return lax.dynamic_slice(saved_input, (0, start), (saved_input.shape[0], size))

    pair_input = swap(input_cols((1 - core) * half_rows, half_rows), "dp", 1)
    att, grad_values = probs_and_grad_values(queries, keys, grad_attended)
    others = [swap(grad_values, "tensor", j) for j in range(1, nt)]
    all_grads = jnp.concatenate([grad_values] + others, axis=1)

    for level in range(levels):
        for half, order in enumerate(orders):
            bit = order[levels - 1 - level]
            own = shards[half]
            other = swap(own, "dp", 1 << bit)
            b = (d >> bit) & 1
            shards[half] = jnp.concatenate([pick(b, own, other), pick(b, other, own)], axis=0)
    received = [swap(own, "dp", 1) for own in shards]

    pair_grads = swap(all_grads, "dp", 1)
    home = input_cols(core * half_rows, half_rows)
    summed = dot(home, all_grads, 0, 0)
    summed = (summed + dot(pair_input, pair_grads, 0, 0)).astype(BF16)
    tiles = []
    for half, order in enumerate(orders):
        part = summed[half * quarter : (half + 1) * quarter]
        columns = {j: part[:, j * width : (j + 1) * width] for j in range(nt)}
        flip = (nt - 1) if half else 0
        chunks = {p: columns[p ^ flip] for p in range(nt)}
        for bit in order:
            b = (d >> bit) & 1
            mask = 1 << (bit - 1)
            lows = sorted(p for p in chunks if not p & mask)
            give = jnp.concatenate([pick(b, chunks[p | mask], chunks[p]) for p in lows], axis=1)
            got = swap(give.astype(BF16), "dp", 1 << bit).astype(F32)
            chunks = {
                p: pick(b, chunks[p], chunks[p | mask]).astype(F32)
                + got[:, i * width : (i + 1) * width]
                for i, p in enumerate(lows)
            }
        (tile,) = chunks.values()
        route = []
        for di in range(nd):
            for ti in range(nt):
                to = (2 * ti + (di & 1)) * nt + ((di >> 1) ^ ti ^ flip)
                route.append((di * nt + ti, to))
        tiles.append(lax.ppermute(tile.astype(BF16), ("dp", "tensor"), route))
    grad_value_weight = jnp.concatenate(tiles, axis=0).astype(F32) / F32(nd)

    own_starts = [half * half_rows + core * quarter for half in range(2)]
    pair_starts = [half * half_rows + (1 - core) * quarter for half in range(2)]
    partial = sum(dot(input_cols(s, quarter), w, 1, 0) for s, w in zip(own_starts, shards))
    partial += sum(dot(input_cols(s, quarter), w, 1, 0) for s, w in zip(pair_starts, received))
    partial = partial.astype(BF16)
    parts = []
    for j in range(nt):
        block = partial[:, j * width : (j + 1) * width]
        parts.append(block if j == 0 else swap(block, "tensor", j))
    grad_queries, grad_keys = query_key_grads(att, queries, keys, grad_attended, parts)

    pieces = []
    for own_w, pair_w in zip(shards, received):
        own = dot(all_grads, own_w, 1, 1).astype(BF16)
        pair = dot(all_grads, pair_w, 1, 1).astype(BF16)
        pieces += [pick(core, own, pair), pick(core, pair, own)]
    grad_input = jnp.concatenate(pieces, axis=1)
    return grad_input, grad_value_weight, grad_queries, grad_keys


def by_collectives(saved_input, queries, keys, value_weight, grad_attended):
    full_input = lax.all_gather(saved_input, "tensor", axis=1, tiled=True)
    att, grad_values = probs_and_grad_values(queries, keys, grad_attended)
    weight_part = dot(full_input, grad_values, 0, 0).astype(BF16)
    summed = lax.psum_scatter(weight_part, "dp", scatter_dimension=0, tiled=True).astype(F32)
    input_part = dot(grad_values, value_weight, 1, 1).astype(BF16)
    grad_input = lax.psum_scatter(input_part, "tensor", scatter_dimension=1, tiled=True)
    values = dot(full_input, value_weight, 1, 0)
    grad_queries, grad_keys = query_key_grads(att, queries, keys, grad_attended, [values])
    return grad_input, summed / F32(lax.axis_size("dp")), grad_queries, grad_keys


def solution(mesh):
    nd, nt = mesh.shape["dp"], mesh.shape["tensor"]

    def on_device(saved_input, *rest):
        paired = nd == 2 * nt and nt > 1 and nt & (nt - 1) == 0
        if paired and saved_input.shape[1] % (32 * nd) == 0:
            return by_shared_weights(saved_input, *rest)
        return by_collectives(saved_input, *rest)

    split = P("dp", "tensor")
    return jax.shard_map(
        on_device,
        mesh=mesh,
        in_specs=(split, split, split, P(None, "tensor"), split),
        out_specs=(split, split, split, split),
        check_vma=False,
    )
```
